32 devices in a mesh: grp: 4 (over y, x), seq: 8 (over z, core).
Axes of the slice: x: 2, y: 2, z: 4, core: 2. Of those that a mesh axis runs over, the one named last changes fastest.
Arguments:
- queries: bfloat16 [8192, 2048], P(('grp', 'seq')), may hold values from -48 to 48
- key_rows: bfloat16 [8192, 512], P(('grp', 'seq')), may hold values from -4.5 to 4.5
- value_rows: bfloat16 [8192, 512], P(('grp', 'seq')), may hold values from -6 to 6
- segments: int32 [8192], P(('grp', 'seq')), may hold values from 0 to 3, as said below
Outputs:
- attended: bfloat16 [8192, 2048], P(('grp', 'seq'))
- log_sums: float32 [16, 8192], P(None, ('grp', 'seq'))
The draws below stay inside these ranges and needn't reach their ends.
Inputs may be any that keep to these rules, and one draw needn't show every extreme that they name: `segments`: never falls along the sequence, starts at 0 and rises by one at each new document; the last token holds the largest value.
All inputs are finite; a program needn't handle non-finite values.
Results may differ from the reference program's by a relative error of at most 0.0035.
Values may be sent and summed in bfloat16 or wider, within the bound.
A program may use at most 192 MiB of HBM per device.

```python
import math
import jax
import jax.numpy as jnp
from jax import lax

Q_HEADS = 16
KV_HEADS = 4
HEAD_DIM = 128
WINDOW = 4096
TOK_DEV = 256
SEQ_LEN = 8192


def boundary_flags(key):
    stretch = max(WINDOW // 2, 2)
    pieces = SEQ_LEN // stretch
    offsets = jax.random.randint(jax.random.fold_in(key, 11), (pieces,), 1, stretch)
    spots = jnp.arange(SEQ_LEN)
    first_mark = SEQ_LEN // 2 - TOK_DEV // 2
    second_mark = SEQ_LEN // 2 + TOK_DEV // 2
    low_piece = first_mark // stretch
    high_piece = min(pieces - 1, (second_mark + WINDOW) // stretch)
    piece_of = spots // stretch
    kept = (piece_of < low_piece) | (piece_of > high_piece)
    flags = (kept & (spots % stretch == offsets[piece_of])).astype(jnp.int32)
    flags = jnp.where((spots == first_mark) | (spots == second_mark), 1, flags)
    return flags.at[0].set(0)


def draw_segments(key, part):
    return jnp.cumsum(boundary_flags(key)).astype(jnp.int32)


def query_key_pair(key):
    group = Q_HEADS // KV_HEADS
    keys = jnp.clip(jax.random.normal(jax.random.fold_in(key, 21), (SEQ_LEN, KV_HEADS, HEAD_DIM), jnp.float32), -4.5, 4.5)
    queries = jnp.clip(3.0 * jax.random.normal(jax.random.fold_in(key, 22), (SEQ_LEN, KV_HEADS, group, HEAD_DIM), jnp.float32), -18.0, 18.0)
    return (queries.reshape(SEQ_LEN, Q_HEADS * HEAD_DIM).astype(jnp.bfloat16), keys.reshape(SEQ_LEN, KV_HEADS * HEAD_DIM).astype(jnp.bfloat16))


def draw_queries(key, part):
    return query_key_pair(key)[0]


def draw_key_rows(key, part):
    return query_key_pair(key)[1]


def steps_of(rng, extent, split, least, top_value):
    gain, own = 1.0, jax.random.fold_in(rng, 6)
    for position, blocks in split:
        heights = jnp.exp(jax.random.uniform(jax.random.fold_in(own, position), (blocks,), jnp.float32, least / len(split), top_value / len(split)))
        gain = gain * jnp.repeat(heights, extent[position] // blocks).reshape([-1 if axis == position else 1 for axis in range(len(extent))])
    return gain


def centred(key, dims, deviation, bound, cuts=(), kind=jnp.bfloat16):
    entries = jax.random.normal(key, dims, jnp.float32) * deviation
    if len(cuts) > 0:
        entries = steps_of(key, dims, cuts, -0.22, 0.18) * entries
    return jnp.clip(entries, min=-bound, max=bound).astype(kind)


def setup_inputs(seed: int = 0) -> dict:
    splits = jax.random.split(jax.random.key(seed), 5)
    return {
        "queries": draw_queries(jax.random.fold_in(splits[4], 71), 0),
        "key_rows": draw_key_rows(jax.random.fold_in(splits[4], 71), 0),
        "value_rows": centred(splits[2], (SEQ_LEN, KV_HEADS * HEAD_DIM), 1.0, 6.0, ((0, 32),)),
        "segments": draw_segments(jax.random.fold_in(splits[4], 71), 0),
    }


def reference(queries, key_rows, value_rows, segments):
    group = Q_HEADS // KV_HEADS
    block = math.gcd(SEQ_LEN, 512)
    count = SEQ_LEN // block
    span = block + WINDOW
    scale = 1.0 / math.sqrt(HEAD_DIM)
    width = KV_HEADS * HEAD_DIM
    key_pad = jnp.concatenate([jnp.zeros((WINDOW, width), key_rows.dtype), key_rows], axis=0)
    value_pad = jnp.concatenate([jnp.zeros((WINDOW, width), value_rows.dtype), value_rows], axis=0)
    seg_pad = jnp.concatenate([jnp.full((WINDOW,), -1, jnp.int32), segments.astype(jnp.int32)], axis=0)

    def one_block(index):
        first = (index * block).astype(jnp.int32)
        q_part = lax.dynamic_slice_in_dim(queries, first, block, 0).reshape(block, KV_HEADS, group, HEAD_DIM).astype(jnp.float32)
        k_part = lax.dynamic_slice_in_dim(key_pad, first, span, 0).reshape(span, KV_HEADS, HEAD_DIM).astype(jnp.float32)
        v_part = lax.dynamic_slice_in_dim(value_pad, first, span, 0).reshape(span, KV_HEADS, HEAD_DIM).astype(jnp.float32)
        q_seg = lax.dynamic_slice_in_dim(segments.astype(jnp.int32), first, block, 0)
        k_seg = lax.dynamic_slice_in_dim(seg_pad, first, span, 0)
        q_pos = first + jnp.arange(block, dtype=jnp.int32)
        k_pos = first - WINDOW + jnp.arange(span, dtype=jnp.int32)
        allowed = (k_pos[None, :] <= q_pos[:, None]) & (k_pos[None, :] > q_pos[:, None] - WINDOW) & (k_seg[None, :] == q_seg[:, None])
        scores = jnp.einsum('tkgd,lkd->kgtl', q_part, k_part, precision=lax.Precision.HIGHEST) * scale
        masked = jnp.where(allowed, scores, -1e+30)
        top = lax.optimization_barrier(jnp.max(masked, axis=-1))
        expo = jnp.where(allowed, jnp.exp(masked - top[..., None]), 0.0)
        total = lax.optimization_barrier(jnp.sum(expo, axis=-1))
        weights = lax.optimization_barrier(expo.astype(jnp.bfloat16))
        summed = jnp.einsum('kgtl,lkd->tkgd', weights.astype(jnp.float32), v_part, precision=lax.Precision.HIGHEST)
        out = summed / jnp.transpose(total, (2, 0, 1))[..., None]
        out = out.reshape(block, Q_HEADS * HEAD_DIM).astype(jnp.bfloat16)
        sums = (top + jnp.log(total)).reshape(Q_HEADS, block)
        return (out, sums)
    outs, sums = lax.map(one_block, jnp.arange(count, dtype=jnp.int32))
    attended = outs.reshape(SEQ_LEN, Q_HEADS * HEAD_DIM)
    log_sums = jnp.transpose(sums, (1, 0, 2)).reshape(Q_HEADS, SEQ_LEN)
    return (attended, log_sums)
```

```python
import functools
import heapq
import math

import jax
import jax.numpy as jnp
from jax import lax
from jax.experimental import pallas as pl
from jax.experimental.pallas import tpu as pltpu
from jax.sharding import PartitionSpec as P

Q_HEADS = 16
KV_HEADS = 4
HEAD_DIM = 128
WINDOW = 4096
AXES = ("grp", "seq")
LOW = -1e30


def block_step(qt, k_ref, v_ref, m_ref, l_ref, acc, bias):
    c = math.log2(math.e) / math.sqrt(HEAD_DIM)
    group = Q_HEADS // KV_HEADS

    def scores(h):
        g = h // group
        return jnp.dot(
            k_ref[:, g * HEAD_DIM : (g + 1) * HEAD_DIM], qt[h], preferred_element_type=jnp.float32
        )

    def summed(h, p, alpha):
        g = h // group
        if h % group == 0:
            vts[g] = v_ref[:, g * HEAD_DIM : (g + 1) * HEAD_DIM].T
        acc[h] = acc[h] * alpha + jnp.dot(vts[g], p, preferred_element_type=jnp.float32)

    vts = {}
    AHEAD = 2
    ready = [scores(h) for h in range(AHEAD)]
    waiting = None
    for h in range(Q_HEADS):
        if h + AHEAD < Q_HEADS:
            ready.append(scores(h + AHEAD))
        s = ready.pop(0)
        if bias is not None:
            s = s + bias[...]
        m_old = m_ref[h]
        m_new = jnp.maximum(m_old, jnp.max(s, axis=0, keepdims=True))
        p = jnp.exp2((s - m_new) * c)
        alpha = jnp.exp2((m_old - m_new) * c)
        l_ref[h] = l_ref[h] * alpha + jnp.sum(p, axis=0, keepdims=True)
        m_ref[h] = m_new
        if waiting is not None:
            summed(*waiting)
        waiting = (h, p.astype(jnp.bfloat16), alpha)
    summed(*waiting)


def flash(info, lower_ref, q_ref, k_ref, v_ref, o_ref, ls_ref, qt, m_ref, l_ref, acc, bias):
    j = pl.program_id(0)
    tok = q_ref.shape[0]
    device, first, clean = info[0], info[1], info[2]

    @pl.when(j == 0)
    def _():
        for h in range(Q_HEADS):
            qt[h] = q_ref[:, h * HEAD_DIM : (h + 1) * HEAD_DIM].T
        m_ref[...] = jnp.full_like(m_ref, LOW)
        l_ref[...] = jnp.zeros_like(l_ref)
        acc[...] = jnp.zeros_like(acc)

    block = device - j
    edge = (j == 0) | (block < clean)

    @pl.when((block >= first) & edge)
    def _():
        key_pos = block * tok + lax.broadcasted_iota(jnp.int32, (tok, tok), 0)
        pos = device * tok + lax.broadcasted_iota(jnp.int32, (tok, tok), 1)
        allowed = (key_pos >= lower_ref[...]) & (key_pos <= pos)
        bias[...] = jnp.where(allowed, 0.0, LOW)
        block_step(qt, k_ref, v_ref, m_ref, l_ref, acc, bias)

    @pl.when((block >= first) & jnp.logical_not(edge))
    def _():
        block_step(qt, k_ref, v_ref, m_ref, l_ref, acc, None)

    @pl.when(j == pl.num_programs(0) - 1)
    def _():
        for h in range(Q_HEADS):
            out = acc[h] * (1.0 / l_ref[h])
            o_ref[:, h * HEAD_DIM : (h + 1) * HEAD_DIM] = out.T.astype(o_ref.dtype)
            ls_ref[h : h + 1, :] = m_ref[h] * (1.0 / math.sqrt(HEAD_DIM)) + jnp.log(l_ref[h])


def routes(n, c, z, g, s, j):
    other = z + 1 - 2 * (z % 2)
    cross = not (s == other and j == 1)
    near, far = s == 1 and j == 1, s == n - 1 and j == 1
    up, down = z + 1 < n and s <= z, z > 0 and s >= z
    out = []
    if c in (0, 2) and g == c:
        if up:
            out.append(0)
        if down and not (c == 2 and z == 1 and (near or far)):
            out.append(1)
        if cross and not (c == 2 and z == 0 and far):
            out.append(2)
        if c == 0 and s >= z and not (z == 0 and near):
            out.append(3)
    elif c == 0 and g == 1:
        out.append(3)
    elif c == 1 and g == 1:
        if up:
            out.append(0)
        if down:
            out.append(1)
        if s < z and j == 1:
            out.append(2)
        elif not (z == 0 and near):
            out.append(3)
    elif c in (1, 3) and g == c - 1:
        if s == z and j == 1:
            out.append(z % 2)
        elif c == 3 and z == 1 and far:
            out.append(1)
    elif c == 2:
        if g == 0 and z == 1 and near:
            out.append(1)
        if g == 1 and (z in (1, n - 2) and far or z == 1 and s == n - 1):
            out.append(1)
    elif c == 3 and g == 3:
        if up:
            out.append(0)
    elif c == 3 and g == 1:
        if not (z <= 1 and far or z == 0 and s == n - 1):
            out.append(2)
        if z == 1 and near:
            out.append(1)
    return out


def step_to(c, z, d):
    return ((c, z + 1), (c, z - 1), (c ^ 1, z), (c ^ 2, z))[d]


def needed(c, z, g, s):
    return (g == c and s <= z) or g == c - 1 or (g == c - 2 and s >= z)


LOCAL, SIBLING, LINK, SEND, COMPUTE = range(5)


def schedule(n, chunk=2.95, flight=1.7, work=1.8, ahead=2.5, ready=4.5):
    chips = [(c, z) for c in range(4) for z in range(n)]

    @functools.lru_cache(None)
    def depth(c, z, g, s, j):
        return max((1 + depth(*step_to(c, z, d), g, s, j) for d in routes(n, c, z, g, s, j)), default=0)

    free, seen, inbox, pend, have, clock, prog, todo = {}, {}, {}, {}, {}, {}, {}, {}
    order = 0
    for c, z in chips:
        ch = c, z
        own = [(2.0 + 1.5 * b, -j, (c, z, j, b)) for b in (0, 1) for j in (1, 0)]
        inbox[ch], have[ch], clock[ch], prog[ch], todo[ch] = own, [], 2.0, [], []
        seen[ch] = [u for _, _, u in own]
        for d in range(4):
            free[ch, d], pend[ch, d] = 0.0, []

    def issue(ch, d, t):
        u = heapq.heappop(pend[ch, d])[2]
        to = step_to(*ch, d)
        free[ch, d] = max(free[ch, d], t) + chunk
        assert u not in seen[to]
        seen[to].append(u)
        heapq.heappush(inbox[to], (free[ch, d] + flight, 0, u))
        return u

    def options(ch):
        t = clock[ch]
        for d in range(4):
            if pend[ch, d]:
                yield max(t, free[ch, d] - ahead), 0, ch, d
        if inbox[ch]:
            yield max(t, inbox[ch][0][0]), 1, ch, 0
        if todo[ch]:
            yield max(t, ready), 2, ch, 0

    while True:
        best = min((o for ch in chips for o in options(ch)), default=None)
        if best is None:
            break
        t, kind, ch, d = best
        if kind == 0:
            prog[ch].append((SEND, issue(ch, d, t), 1 << d))
            clock[ch] = t + 0.05
        elif kind == 1:
            u = heapq.heappop(inbox[ch])[2]
            g, s, j, b = u
            mask = 0
            for d in routes(n, *ch, g, s, j):
                order += 1
                heapq.heappush(pend[ch, d], (-depth(*step_to(*ch, d), g, s, j), order, u))
                if free[ch, d] - ahead <= t and pend[ch, d][0][2] == u:
                    issue(ch, d, t)
                    mask |= 1 << d
            op = LINK if (g, s) != ch else (LOCAL, SIBLING)[b]
            prog[ch].append((op, u, mask))
            clock[ch] = t + 0.1
            have[ch].append(u)
            if needed(*ch, g, s) and (g, s, j, 1 - b) in have[ch]:
                todo[ch].append((g, s, j, 0))
        else:
            todo[ch].sort(key=lambda u: (u[0], u[1]) != ch)
            prog[ch].append((COMPUTE, todo[ch].pop(0), 0))
            clock[ch] = max(t, ready) + work
    for ch in chips:
        done = [u[:3] for op, u, _ in prog[ch] if op == COMPUTE]
        want = [(g, s, j) for g in range(4) for s in range(n) for j in range(2) if needed(*ch, g, s)]
        assert sorted(done) == want

    def word(op, u, mask):
        g, s, j, b = u
        return op + 8 * (b + 2 * (mask + 16 * ((g * n + s) * 2 + j)))

    moves, stops, works = [], [], []
    for ch in chips:
        stop, work = [], []
        for op, u, _ in prog[ch]:
            if op == COMPUTE:
                stop.append(len([e for e in prog[ch][: prog[ch].index((op, u, 0))] if e[0] != COMPUTE]))
                work.append((u[0] * n + u[1]) * 2 + u[2])
        move = [word(*e) for e in prog[ch] if e[0] != COMPUTE]
        moves.append(move)
        stops.append(stop + [len(move)])
        works.append(work)
    steps = max(len(w) for w in works)
    counts = [len(w) for w in works]
    stops = [s[:-1] + [s[-1]] * (steps + 1 - len(s) + 1) for s in stops]
    works = [w + [w[-1]] * (steps - len(w)) for w in works]
    return moves, stops, works, counts


def pick(words, bits):
    for bit in bits:
        if len(words) == 1:
            break
        pairs = [(words[i], words[min(i + 1, len(words) - 1)]) for i in range(0, len(words), 2)]
        words = [
            lo if isinstance(lo, int) and isinstance(hi, int) and lo == hi else jnp.where(bit, jnp.int32(hi), jnp.int32(lo))
            for lo, hi in pairs
        ]
    return words[0]


def exchange_attend(n, k_in, v_in, q_in, seg_in, o_out, ls_out, table, ends, c_in, s_in, kv, qraw, segs, qt, m_ref, acc, obuf, lsbuf, seg_here,
                    local, sib_send, sib_recv, link_send, link_recv):
    tok = k_in.shape[0]
    heads = Q_HEADS // 2
    group = Q_HEADS // KV_HEADS
    scale = math.log2(math.e) / math.sqrt(HEAD_DIM)
    c, s = lax.axis_index("grp"), lax.axis_index("seq")
    z, k = lax.div(s, 2), lax.rem(s, 2)
    sib = s + 1 - 2 * k
    row, col = lax.div(c, 2), lax.rem(c, 2)
    peers = (
        (z + 1 < n, (c, s + 2)),
        (z > 0, (c, s - 2)),
        (c >= 0, (c + 1 - 2 * col, s)),
        (c >= 0, (c + 2 - 4 * row, s)),
        (c >= 0, (c, sib)),
    )
    here = (c * n + z) * 2

    def parts(core):
        made = []
        for j in range(2):
            cols = pl.ds(pl.multiple_of((2 * core + j) * HEAD_DIM, HEAD_DIM), HEAD_DIM)
            for t, src in enumerate((k_in.at[:, cols], v_in.at[:, cols], c_in)):
                rows = pl.ds(t * tok, src.shape[0])
                made.append((src, kv.at[here + j, k, rows, :], 3 * j + t))
        cols = pl.ds(pl.multiple_of(core * heads * HEAD_DIM, HEAD_DIM), heads * HEAD_DIM)
        made.append((q_in.at[:, cols], qraw.at[k], 6))
        made.append((s_in, segs.at[k], 7))
        return made

    def to_sib(src, dst, i):
        return pltpu.make_async_remote_copy(
            src_ref=src, dst_ref=dst, send_sem=sib_send.at[i], recv_sem=sib_recv.at[i],
            device_id=(c, sib), device_id_type=pl.DeviceIdType.MESH,
        )

    mine = {i: pltpu.make_async_copy(src, dst, local.at[i]) for src, dst, i in parts(k) if i in (0, 1, 3, 4, 6)}
    theirs = [to_sib(src, dst, i) for src, dst, i in parts(1 - k)]

    def coming(j, t):
        rows = pl.ds(t * tok, tok if t < 2 else c_in.shape[0])
        ref = kv.at[here + j, 1 - k, rows, :]
        return to_sib(ref, ref, 3 * j + t)

    fetch = pltpu.make_async_copy(seg_in, seg_here, local.at[7])
    fetch.start()
    for copy in mine.values():
        copy.start()
    barrier = pltpu.get_barrier_semaphore()
    count = 0
    for ok, to in peers:
        count = count + ok.astype(jnp.int32)

        @pl.when(ok)
        def _(to=to):
            pl.semaphore_signal(barrier, inc=1, device_id=to, device_id_type=pl.DeviceIdType.MESH)

    moves, stops, works, counts = schedule(n)
    for i in range(len(moves)):

        @pl.when(c * n + z == i)
        def _(i=i):
            for e, w in enumerate(moves[i]):
                table[e] = w
            for e, w in enumerate(stops[i]):
                ends[e] = w

    bits = [lax.rem(lax.div(c * n + z, 2**i), 2) == 1 for i in range(4)]
    steps = len(works[0])
    units = [pick([w[t] for w in works], bits) for t in range(steps)]
    active = pick(counts, bits)

    fetch.wait()
    seg = seg_here[...].astype(jnp.float32)
    docs = lax.broadcasted_iota(jnp.int32, (HEAD_DIM, tok), 0).astype(jnp.float32)
    before = jnp.where(seg < docs, 1.0, 0.0).astype(jnp.bfloat16)
    counted = lax.dot_general(
        jnp.ones((16, tok), jnp.bfloat16), before, (((1,), (1,)), ((), ())), preferred_element_type=jnp.float32
    ).astype(jnp.bfloat16)
    wide = jnp.broadcast_to(seg, (16, tok)).astype(jnp.bfloat16)
    c_in[...] = counted
    s_in[...] = wide
    segs[k] = wide
    for j in range(2):
        kv[here + j, k, 2 * tok : 2 * tok + 16, :] = counted
    m_ref[...] = jnp.full_like(m_ref, LOW)
    acc[...] = jnp.zeros_like(acc)
    pl.semaphore_wait(barrier, count)
    for copy in theirs:
        copy.start()

    def link(d, unit, b):
        return pltpu.make_async_remote_copy(
            src_ref=kv.at[unit, b], dst_ref=kv.at[unit, b],
            send_sem=link_send.at[d, unit, b], recv_sem=link_recv.at[unit, b],
            device_id=peers[d][1], device_id_type=pl.DeviceIdType.MESH,
        )

    def decode(e):
        w = table[e]
        op, w = lax.rem(w, 8), lax.div(w, 8)
        b, w = lax.rem(w, 2), lax.div(w, 2)
        mask, unit = lax.rem(w, 16), lax.div(w, 16)
        return op, lax.rem(b + k, 2), mask, unit

    def query_block(b):
        onehot = lax.broadcasted_iota(jnp.int32, (HEAD_DIM, tok), 0).astype(jnp.float32)
        onehot = (segs[b, 0:1, :].astype(jnp.float32) == onehot).astype(jnp.bfloat16)
        at = slice(b * tok, (b + 1) * tok)
        for h in range(heads):
            qt[h, 0:HEAD_DIM, at] = qraw[b, :, h * HEAD_DIM : (h + 1) * HEAD_DIM].T
            qt[h, HEAD_DIM:, at] = onehot

    def body(unit, masked):
        j = lax.rem(unit, 2)
        keys, values = [], []
        for b in range(2):
            counts = kv[unit, b, 2 * tok : 2 * tok + 1, :].astype(jnp.float32)
            at = lax.broadcasted_iota(jnp.int32, (tok, HEAD_DIM), 0).astype(jnp.float32)
            shut = jnp.where(at < counts, LOW, 0.0).astype(jnp.bfloat16)
            keys.append(jnp.concatenate([kv[unit, b, 0:tok, :], shut], axis=1))
            vt = kv[unit, b, tok : 2 * tok, :].T
            values.append(jnp.concatenate([vt, jnp.ones((16, tok), jnp.bfloat16)], axis=0))
        tiles = [(i, q) for i in range(group) for q in range(2)]

        def scores(i, q):
            right = qt[group * j + i, :, q * tok : (q + 1) * tok]
            return [jnp.dot(keys[b], right, preferred_element_type=jnp.float32) for b in range(2)]

        def summed(i, q, ps, alpha):
            pv = sum(jnp.dot(values[b], ps[b], preferred_element_type=jnp.float32) for b in range(2))
            at = slice(q * tok, (q + 1) * tok)
            acc[group * j + i, :, at] = acc[group * j + i, :, at] * alpha + pv

        AHEAD = 2
        ready = [scores(*u) for u in tiles[:AHEAD]]
        waiting = None
        for pos, (i, q) in enumerate(tiles):
            if pos + AHEAD < len(tiles):
                ready.append(scores(*tiles[pos + AHEAD]))
            ss = ready.pop(0)
            if masked is not None:
                sign, shift = masked
                diff = lax.broadcasted_iota(jnp.int32, (tok, tok), 0) - lax.broadcasted_iota(jnp.int32, (tok, tok), 1)
                ss = [jnp.where(sign * (diff + (b - q) * tok) + shift <= 0, ss[b], LOW) for b in range(2)]
            at = slice(q * tok, (q + 1) * tok)
            m_old = m_ref[group * j + i, :, at]
            m_new = m_old
            for x in ss:
                m_new = jnp.maximum(m_new, jnp.max(x, axis=0, keepdims=True))
            ps = [jnp.exp2((x - m_new) * scale).astype(jnp.bfloat16) for x in ss]
            alpha = jnp.exp2((m_old - m_new) * scale)
            m_ref[group * j + i, :, at] = m_new
            if waiting is not None:
                summed(*waiting)
            waiting = (i, q, ps, alpha)
        summed(*waiting)

    def entry(e, carry):
        op, b, mask, unit = decode(e)

        @pl.when(op == LOCAL)
        def _():
            for j in range(2):

                @pl.when(unit == here + j)
                def _(j=j):
                    for t in range(2):
                        mine[3 * j + t].wait()

        @pl.when(op == SIBLING)
        def _():
            for j in range(2):

                @pl.when(unit == here + j)
                def _(j=j):
                    for t in range(3):
                        coming(j, t).wait_recv()

        @pl.when(op == LINK)
        def _():
            link(0, unit, b).wait_recv()

        for d in range(4):

            @pl.when(lax.rem(lax.div(mask, 2**d), 2) == 1)
            def _(d=d):
                link(d, unit, b).start()

        return carry

    def step(t, carry):
        lax.fori_loop(jnp.where(t == 0, first, ends[jnp.maximum(t - 1, 0)]), ends[t], entry, 0)
        unit = pick(units, [lax.rem(lax.div(t, 2**i), 2) == 1 for i in range(steps.bit_length())])
        slab = lax.div(unit, 2)
        back, at = c - lax.div(slab, n), lax.rem(slab, n)
        rim = (at == z) & ((back == 0) | (back == 2))

        @pl.when((t < active) & rim)
        def _():
            sign = jnp.where(back == 0, 1, -1)
            body(unit, (sign, jnp.where(back == 0, 0, 1)))

        @pl.when((t < active) & jnp.logical_not(rim))
        def _():
            body(unit, None)

        return carry

    first = 4
    lax.fori_loop(0, first, entry, 0)
    mine[6].wait()
    for i in (6, 7):
        ref = (qraw, segs)[i - 6].at[1 - k]
        to_sib(ref, ref, i).wait_recv()
    for b in range(2):
        query_block(b)
    lax.fori_loop(0, steps, step, 0)
    lax.fori_loop(ends[steps - 1], ends[steps], entry, 0)

    for h in range(heads):
        total = acc[h, HEAD_DIM : HEAD_DIM + 1, :]
        out = acc[h, 0:HEAD_DIM, :] * (1.0 / total)
        logs = m_ref[h] * (1.0 / math.sqrt(HEAD_DIM)) + jnp.log(total)
        for b in range(2):
            at = slice(b * tok, (b + 1) * tok)
            obuf[b, :, h * HEAD_DIM : (h + 1) * HEAD_DIM] = out[:, at].T.astype(obuf.dtype)
            lsbuf[b, h : h + 1, :] = logs[:, at]
    cols = pl.ds(pl.multiple_of(k * heads * HEAD_DIM, HEAD_DIM), heads * HEAD_DIM)
    rows = pl.ds(pl.multiple_of(k * heads, heads), heads)
    back = [to_sib(obuf.at[1 - k], o_out.at[:, cols], 8), to_sib(lsbuf.at[1 - k], ls_out.at[rows, :], 9)]
    keep = [
        pltpu.make_async_copy(obuf.at[k], o_out.at[:, cols], local.at[8]),
        pltpu.make_async_copy(lsbuf.at[k], ls_out.at[rows, :], local.at[9]),
    ]
    for copy in back + keep:
        copy.start()

    def finish(e, carry):
        _, b, mask, unit = decode(e)
        for d in range(4):

            @pl.when(lax.rem(lax.div(mask, 2**d), 2) == 1)
            def _(d=d):
                link(d, unit, b).wait_send()

        return carry

    lax.fori_loop(0, ends[steps], finish, 0)
    for copy in theirs + back:
        copy.wait_send()
    other = pl.ds(pl.multiple_of((1 - k) * heads * HEAD_DIM, HEAD_DIM), heads * HEAD_DIM)
    low = pl.ds(pl.multiple_of((1 - k) * heads, heads), heads)
    to_sib(obuf.at[k], o_out.at[:, other], 8).wait_recv()
    to_sib(lsbuf.at[k], ls_out.at[low, :], 9).wait_recv()
    for copy in keep:
        copy.wait()


def fused(queries, key_rows, value_rows, segments):
    n = lax.axis_size("seq") // 2
    tok = queries.shape[0]
    heads = Q_HEADS // 2
    hbm = pl.BlockSpec(memory_space=pltpu.HBM)
    units = 8 * n
    moves, stops, _, _ = schedule(n)
    return pl.pallas_call(
        functools.partial(exchange_attend, n),
        out_shape=[
            jax.ShapeDtypeStruct(queries.shape, jnp.bfloat16),
            jax.ShapeDtypeStruct((Q_HEADS, tok), jnp.float32),
        ],
        in_specs=[hbm] * 4,
        out_specs=[pl.BlockSpec(memory_space=pl.ANY)] * 2,
        scratch_shapes=[
            pltpu.SMEM((max(len(m) for m in moves),), jnp.int32),
            pltpu.SMEM((len(stops[0]),), jnp.int32),
            pltpu.VMEM((16, HEAD_DIM), jnp.bfloat16),
            pltpu.VMEM((16, tok), jnp.bfloat16),
            pltpu.VMEM((units, 2, 2 * tok + 16, HEAD_DIM), jnp.bfloat16),
            pltpu.VMEM((2, tok, heads * HEAD_DIM), jnp.bfloat16),
            pltpu.VMEM((2, 16, tok), jnp.bfloat16),
            pltpu.VMEM((heads, 2 * HEAD_DIM, 2 * tok), jnp.bfloat16),
            pltpu.VMEM((heads, 1, 2 * tok), jnp.float32),
            pltpu.VMEM((heads, HEAD_DIM + 16, 2 * tok), jnp.float32),
            pltpu.VMEM((2, tok, heads * HEAD_DIM), jnp.bfloat16),
            pltpu.VMEM((2, heads, tok), jnp.float32),
            pltpu.VMEM((1, tok), jnp.int32),
            pltpu.SemaphoreType.DMA((10,)),
            pltpu.SemaphoreType.DMA((10,)),
            pltpu.SemaphoreType.DMA((10,)),
            pltpu.SemaphoreType.DMA((4, units, 2)),
            pltpu.SemaphoreType.DMA((units, 2)),
        ],
        compiler_params=pltpu.CompilerParams(
            collective_id=0, has_side_effects=True, vmem_limit_bytes=24 * 1024 * 1024
        ),
    )(*(pltpu.with_memory_space_constraint(x, pltpu.HBM) for x in (key_rows, value_rows, queries, segments[None, :])))


def on_device(queries, key_rows, value_rows, segments):
    tok = queries.shape[0]
    grp_n, seq_n = lax.axis_size("grp"), lax.axis_size("seq")
    device = lax.axis_index(AXES)
    offset = device * tok
    if grp_n == 4 and seq_n == 8 and 2 * seq_n * tok == WINDOW and tok <= 256:
        return fused(queries, key_rows, value_rows, segments)
    k_all = lax.all_gather(key_rows, AXES)
    v_all = lax.all_gather(value_rows, AXES)
    seg_all = lax.all_gather(segments, AXES)
    base = 0
    seg_all = seg_all.reshape(-1)
    key_pos = base * tok + jnp.arange(seg_all.shape[0], dtype=jnp.int32)
    begin = jnp.maximum(offset - WINDOW, 0)
    before = (key_pos >= begin) & (key_pos < offset) & (seg_all < segments[0])
    carried = begin + jnp.sum(before.astype(jnp.int32))
    inner = jnp.sum((segments[:, None] < segments[None, :]).astype(jnp.int32), axis=0)
    starts = jnp.where(segments == segments[0], carried, offset + inner)
    positions = offset + jnp.arange(tok, dtype=jnp.int32)
    lower = jnp.maximum(starts, positions - WINDOW + 1)
    first = jnp.min(lower) // tok
    clean = (jnp.max(lower) + tok - 1) // tok
    info = jnp.stack([device, first, clean, device - base]).astype(jnp.int32)
    reach = (WINDOW - 1 + tok - 1) // tok + 1
    return attention(info, lower, queries, k_all, v_all, reach)


def attention(info, lower, queries, k_all, v_all, reach):
    tok = queries.shape[0]
    width = k_all.shape[2]

    def kv_index(j, info):
        return (jnp.maximum(info[3] - j, info[3] - info[0] + info[1]), 0, 0)

    const = lambda j, info: (0, 0)
    return pl.pallas_call(
        flash,
        grid_spec=pltpu.PrefetchScalarGridSpec(
            num_scalar_prefetch=1,
            grid=(reach,),
            in_specs=[
                pl.BlockSpec((1, tok), const),
                pl.BlockSpec(queries.shape, const),
                pl.BlockSpec((None, tok, width), kv_index),
                pl.BlockSpec((None, tok, width), kv_index),
            ],
            out_specs=[
                pl.BlockSpec(queries.shape, const),
                pl.BlockSpec((Q_HEADS, tok), const),
            ],
            scratch_shapes=[
                pltpu.VMEM((Q_HEADS, HEAD_DIM, tok), jnp.bfloat16),
                pltpu.VMEM((Q_HEADS, 1, tok), jnp.float32),
                pltpu.VMEM((Q_HEADS, 1, tok), jnp.float32),
                pltpu.VMEM((Q_HEADS, HEAD_DIM, tok), jnp.float32),
                pltpu.VMEM((tok, tok), jnp.float32),
            ],
        ),
        out_shape=[
            jax.ShapeDtypeStruct(queries.shape, jnp.bfloat16),
            jax.ShapeDtypeStruct((Q_HEADS, tok), jnp.float32),
        ],
        compiler_params=pltpu.CompilerParams(dimension_semantics=("arbitrary",)),
    )(info, lower[None, :], queries, k_all, v_all)


def solution(mesh):
    in_specs = (P(AXES, None), P(AXES, None), P(AXES, None), P(AXES))
    out_specs = (P(AXES, None), P(None, AXES))
    return jax.shard_map(
        on_device, mesh=mesh, in_specs=in_specs, out_specs=out_specs, check_vma=False
    )
```

```python
import functools
import heapq
import math

import jax
import jax.numpy as jnp
from jax import lax
from jax.experimental import pallas as pl
from jax.experimental.pallas import tpu as pltpu
from jax.sharding import PartitionSpec as P

Q_HEADS = 16
KV_HEADS = 4
HEAD_DIM = 128
WINDOW = 4096
AXES = ("grp", "seq")
LOW = -1e30


def block_step(qt, k_ref, v_ref, m_ref, l_ref, acc, bias):
    c = math.log2(math.e) / math.sqrt(HEAD_DIM)
    group = Q_HEADS // KV_HEADS

    def scores(h):
        g = h // group
        return jnp.dot(
            k_ref[:, g * HEAD_DIM : (g + 1) * HEAD_DIM], qt[h], preferred_element_type=jnp.float32
        )

    def summed(h, p, alpha):
        g = h // group
        if h % group == 0:
            vts[g] = v_ref[:, g * HEAD_DIM : (g + 1) * HEAD_DIM].T
        acc[h] = acc[h] * alpha + jnp.dot(vts[g], p, preferred_element_type=jnp.float32)

    vts = {}
    AHEAD = 2
    ready = [scores(h) for h in range(AHEAD)]
    waiting = None
    for h in range(Q_HEADS):
        if h + AHEAD < Q_HEADS:
            ready.append(scores(h + AHEAD))
        s = ready.pop(0)
        if bias is not None:
            s = s + bias[...]
        m_old = m_ref[h]
        m_new = jnp.maximum(m_old, jnp.max(s, axis=0, keepdims=True))
        p = jnp.exp2((s - m_new) * c)
        alpha = jnp.exp2((m_old - m_new) * c)
        l_ref[h] = l_ref[h] * alpha + jnp.sum(p, axis=0, keepdims=True)
        m_ref[h] = m_new
        if waiting is not None:
            summed(*waiting)
        waiting = (h, p.astype(jnp.bfloat16), alpha)
    summed(*waiting)


def flash(info, lower_ref, q_ref, k_ref, v_ref, o_ref, ls_ref, qt, m_ref, l_ref, acc, bias):
    j = pl.program_id(0)
    tok = q_ref.shape[0]
    device, first, clean = info[0], info[1], info[2]

    @pl.when(j == 0)
    def _():
        for h in range(Q_HEADS):
            qt[h] = q_ref[:, h * HEAD_DIM : (h + 1) * HEAD_DIM].T
        m_ref[...] = jnp.full_like(m_ref, LOW)
        l_ref[...] = jnp.zeros_like(l_ref)
        acc[...] = jnp.zeros_like(acc)

    block = device - j
    edge = (j == 0) | (block < clean)

    @pl.when((block >= first) & edge)
    def _():
        key_pos = block * tok + lax.broadcasted_iota(jnp.int32, (tok, tok), 0)
        pos = device * tok + lax.broadcasted_iota(jnp.int32, (tok, tok), 1)
        allowed = (key_pos >= lower_ref[...]) & (key_pos <= pos)
        bias[...] = jnp.where(allowed, 0.0, LOW)
        block_step(qt, k_ref, v_ref, m_ref, l_ref, acc, bias)

    @pl.when((block >= first) & jnp.logical_not(edge))
    def _():
        block_step(qt, k_ref, v_ref, m_ref, l_ref, acc, None)

    @pl.when(j == pl.num_programs(0) - 1)
    def _():
        for h in range(Q_HEADS):
            out = acc[h] * (1.0 / l_ref[h])
            o_ref[:, h * HEAD_DIM : (h + 1) * HEAD_DIM] = out.T.astype(o_ref.dtype)
            ls_ref[h : h + 1, :] = m_ref[h] * (1.0 / math.sqrt(HEAD_DIM)) + jnp.log(l_ref[h])


ROUTES = (
    1855310, 1855310, 1758440, 1758565, 4890511576, 9650953, 8464676, 8488425, 42791646, 4929557131, 44727131,
    44816506, 122230363153, 213566280, 213541355, 213542606, 125661521875, 123237693825, 4858872225, 1099025020,
    4608094065, 18200594475, 3659955416, 125683000715, 29780628525, 29780628575, 18034925391, 24382191625,
    133541425450, 144445703125, 151057046875, 130285546875, 114378906250, 114378906250, 82642578125, 108275390625,
    83417968750, 113886718750, 100947656250, 107051171875, 111425781250, 111425781250, 99218750000, 111425781250,
    113049218750, 114269921875, 99121093750, 99121093750, 75683593750, 75683593750, 75683593750, 75683593750,
    73242187500, 73242187500, 73242187500, 73242187500, 61035156250, 61035156250, 61035156250, 61035156250, 0, 0, 0,
    0,
)
EARLY = (
    5, -3, -6.5, -2, 2.5, -5, 9.5, -2.5, -5, -7.5, 2, 9, -4, -6.5, 1, 4.5, -2, -2, 2, 1.5, -3, -0.5, 1, 10.5, 6,
    -5.5, -5.5, 0, -8, -11, -7.5, 6.5, 0.5, 1.5, -4, -10, -3, 2.5, 7.5, 4, -6.5, -5, 1.5, 1.5, -2, -5, 8, 8, -3, 11,
    -0.5, 12, 6.5, -3, 8.5, 0.5, 0, -3.5, 8, -6, 4, 9.5, 3.5, -1.5,
)


def needed(c, z, g, s):
    return (g == c and s <= z) or g == c - 1 or (g == c - 2 and s >= z)


LOCAL, SIBLING, LINK, SEND, COMPUTE = range(5)


def schedule(n, chunk=2.95, flight=1.7, work=1.8, ahead=2.8, ready=5.0):
    chips = [(c, z) for c in range(4) for z in range(n)]
    near = []
    for c, z in chips:
        ways = ((c, z + 1), (c, z - 1), (c ^ 1, z), (c ^ 2, z))
        near.append([chips.index(w) if w in chips else None for w in ways])
    count = len(chips)
    home = [chip for chip in range(count) for _ in range(4)]
    kids, depth = [], []
    for code in ROUTES:
        above = []
        for chip in range(count):
            code, way = divmod(code, 5)
            above.append(near[chip][way - 1] if way else None)
        kid, deep = [[] for _ in chips], [0] * count
        for chip in range(count):
            if above[chip] is not None:
                kid[above[chip]].append(near[above[chip]].index(chip))
                far, hops = chip, 0
                while above[far] is not None:
                    far, hops = above[far], hops + 1
                    deep[far] = max(deep[far], hops)
        kids.append(kid)
        depth.append(deep)

    free = [[0.0] * 4 for _ in chips]
    pend = [[[] for _ in range(4)] for _ in chips]
    inbox = [sorted((2.0 + 1.5 * b, -j, i * 4 + j * 2 + b) for b in (0, 1) for j in (1, 0)) for i in range(count)]
    have, todo, prog = [[] for _ in chips], [[] for _ in chips], [[] for _ in chips]
    clock, order = [2.0] * count, 0

    def option(i):
        found = [(max(free[i][d] - ahead, clock[i]), 0, d) for d in range(4) if pend[i][d]]
        if inbox[i]:
            found.append((max(inbox[i][0][0], clock[i]), 1, 0))
        if todo[i]:
            found.append((max(clock[i], ready), 2, 0))
        return min(found, default=None)

    def issue(i, d, t):
        q = heapq.heappop(pend[i][d])[2]
        to = near[i][d]
        free[i][d] = max(free[i][d], t) + chunk
        heapq.heappush(inbox[to], (free[i][d] + flight, 0, q))
        choice[to] = option(to)
        return q

    choice = [option(i) for i in range(count)]
    while any(o is not None for o in choice):
        t, i = min((o[0], i) for i, o in enumerate(choice) if o is not None)
        _, kind, d = choice[i]
        if kind == 0:
            prog[i].append((SEND, issue(i, d, t), 1 << d))
            clock[i] = t + 0.07
        elif kind == 1:
            q = heapq.heappop(inbox[i])[2]
            mask = 0
            for d in kids[q][i]:
                order += 1
                heapq.heappush(pend[i][d], (-depth[q][near[i][d]] - EARLY[q], order, q))
                if free[i][d] - ahead <= t and pend[i][d][0][2] == q:
                    issue(i, d, t)
                    mask |= 1 << d
            prog[i].append((LINK if home[q] != i else (LOCAL, SIBLING)[q % 2], q, mask))
            clock[i] = t + 0.12
            have[i].append(q)
            if needed(*chips[i], *chips[home[q]]) and q ^ 1 in have[i]:
                todo[i].append(q // 2)
        else:
            todo[i].sort(key=lambda u: u // 2 != i)
            prog[i].append((COMPUTE, todo[i].pop(0) * 2, 0))
            clock[i] = t + work
        choice[i] = option(i)
    for i in range(count):
        assert len(have[i]) == len(set(have[i]))
        done = sorted(q // 2 for op, q, _ in prog[i] if op == COMPUTE)
        assert done == [u for u in range(2 * count) if needed(*chips[i], *chips[u // 2])]

    def word(op, q, mask):
        return op + 8 * (q % 2 + 2 * (mask + 16 * (q // 2)))

    moves, stops, works = [], [], []
    for entries in prog:
        stop, work = [], []
        for place, (op, q, _) in enumerate(entries):
            if op == COMPUTE:
                stop.append(place - len(work))
                work.append(q // 2)
        move = [word(*e) for e in entries if e[0] != COMPUTE]
        moves.append(move)
        stops.append(stop + [len(move)])
        works.append(work)
    steps = max(len(w) for w in works)
    counts = [len(w) for w in works]
    stops = [s[:-1] + [s[-1]] * (steps + 1 - len(s) + 1) for s in stops]
    works = [w + [w[-1]] * (steps - len(w)) for w in works]
    sends = [
        [d + 4 * (w // 8 % 2 + 2 * (w // 256)) for w in move for d in range(4) if w // 16 // 2**d % 2] for move in moves
    ]
    return moves, stops, works, counts, sends


def pick(words, bits):
    for bit in bits:
        if len(words) == 1:
            break
        pairs = [(words[i], words[min(i + 1, len(words) - 1)]) for i in range(0, len(words), 2)]
        words = [
            lo if isinstance(lo, int) and isinstance(hi, int) and lo == hi else jnp.where(bit, jnp.int32(hi), jnp.int32(lo))
            for lo, hi in pairs
        ]
    return words[0]


def exchange_attend(n, k_in, v_in, q_in, seg_in, o_out, ls_out, table, ends, sent, c_in, s_in, kv, qraw, segs, qt, m_ref, acc, obuf, lsbuf, seg_here,
                    local, sib_send, sib_recv, link_send, link_recv):
    tok = k_in.shape[0]
    heads = Q_HEADS // 2
    group = Q_HEADS // KV_HEADS
    scale = math.log2(math.e) / math.sqrt(HEAD_DIM)
    c, s = lax.axis_index("grp"), lax.axis_index("seq")
    z, k = lax.div(s, 2), lax.rem(s, 2)
    sib = s + 1 - 2 * k
    row, col = lax.div(c, 2), lax.rem(c, 2)
    peers = (
        (z + 1 < n, (c, s + 2)),
        (z > 0, (c, s - 2)),
        (c >= 0, (c + 1 - 2 * col, s)),
        (c >= 0, (c + 2 - 4 * row, s)),
        (c >= 0, (c, sib)),
    )
    here = (c * n + z) * 2

    def parts(core):
        made = []
        for j in range(2):
            cols = pl.ds(pl.multiple_of((2 * core + j) * HEAD_DIM, HEAD_DIM), HEAD_DIM)
            for t, src in enumerate((k_in.at[:, cols], v_in.at[:, cols], c_in)):
                rows = pl.ds(t * tok, src.shape[0])
                made.append((src, kv.at[here + j, k, rows, :], 3 * j + t))
        cols = pl.ds(pl.multiple_of(core * heads * HEAD_DIM, HEAD_DIM), heads * HEAD_DIM)
        made.append((q_in.at[:, cols], qraw.at[k], 6))
        made.append((s_in, segs.at[k], 7))
        return made

    def to_sib(src, dst, i):
        return pltpu.make_async_remote_copy(
            src_ref=src, dst_ref=dst, send_sem=sib_send.at[i], recv_sem=sib_recv.at[i],
            device_id=(c, sib), device_id_type=pl.DeviceIdType.MESH,
        )

    mine = {i: pltpu.make_async_copy(src, dst, local.at[i]) for src, dst, i in parts(k) if i in (0, 1, 3, 4, 6)}
    theirs = [to_sib(src, dst, i) for src, dst, i in parts(1 - k)]

    def coming(j, t):
        rows = pl.ds(t * tok, tok if t < 2 else c_in.shape[0])
        ref = kv.at[here + j, 1 - k, rows, :]
        return to_sib(ref, ref, 3 * j + t)

    fetch = pltpu.make_async_copy(seg_in, seg_here, local.at[7])
    fetch.start()
    for copy in mine.values():
        copy.start()
    barrier = pltpu.get_barrier_semaphore()
    count = 0
    for ok, to in peers:
        count = count + ok.astype(jnp.int32)

        @pl.when(ok)
        def _(to=to):
            pl.semaphore_signal(barrier, inc=1, device_id=to, device_id_type=pl.DeviceIdType.MESH)

    moves, stops, works, counts, sends = schedule(n)
    for i in range(len(moves)):

        @pl.when(c * n + z == i)
        def _(i=i):
            for e, w in enumerate(moves[i]):
                table[e] = w
            for e, w in enumerate(stops[i] + [len(sends[i])]):
                ends[e] = w
            for e, w in enumerate(sends[i]):
                sent[e] = w

    bits = [lax.rem(lax.div(c * n + z, 2**i), 2) == 1 for i in range(4)]
    steps = len(works[0])
    units = [pick([w[t] for w in works], bits) for t in range(steps)]
    active = pick(counts, bits)

    fetch.wait()
    seg = seg_here[...].astype(jnp.float32)
    docs = lax.broadcasted_iota(jnp.int32, (HEAD_DIM, tok), 0).astype(jnp.float32)
    before = jnp.where(seg < docs, 1.0, 0.0).astype(jnp.bfloat16)
    counted = lax.dot_general(
        jnp.ones((16, tok), jnp.bfloat16), before, (((1,), (1,)), ((), ())), preferred_element_type=jnp.float32
    ).astype(jnp.bfloat16)
    wide = jnp.broadcast_to(seg, (16, tok)).astype(jnp.bfloat16)
    c_in[...] = counted
    s_in[...] = wide
    segs[k] = wide
    for j in range(2):
        kv[here + j, k, 2 * tok : 2 * tok + 16, :] = counted
    pl.semaphore_wait(barrier, count)
    for copy in theirs:
        copy.start()

    def link(d, unit, b):
        return pltpu.make_async_remote_copy(
            src_ref=kv.at[unit, b], dst_ref=kv.at[unit, b],
            send_sem=link_send.at[d, unit, b], recv_sem=link_recv.at[unit, b],
            device_id=peers[d][1], device_id_type=pl.DeviceIdType.MESH,
        )

    def decode(e):
        w = table[e]
        op, w = lax.rem(w, 8), lax.div(w, 8)
        b, w = lax.rem(w, 2), lax.div(w, 2)
        mask, unit = lax.rem(w, 16), lax.div(w, 16)
        return op, lax.rem(b + k, 2), mask, unit

    def query_block(b):
        onehot = lax.broadcasted_iota(jnp.int32, (HEAD_DIM, tok), 0).astype(jnp.float32)
        onehot = (segs[b, 0:1, :].astype(jnp.float32) == onehot).astype(jnp.bfloat16)
        at = pl.ds(pl.multiple_of(b * tok, HEAD_DIM), tok)
        for h in range(heads):
            qt[h, 0:HEAD_DIM, at] = qraw[b, :, h * HEAD_DIM : (h + 1) * HEAD_DIM].T
            qt[h, HEAD_DIM:, at] = onehot

    def body(unit, masked):
        j = lax.rem(unit, 2)
        keys, values = [], []
        for b in range(2):
            counts = kv[unit, b, 2 * tok : 2 * tok + 1, :].astype(jnp.float32)
            at = lax.broadcasted_iota(jnp.int32, (tok, HEAD_DIM), 0).astype(jnp.float32)
            shut = jnp.where(at < counts, LOW, 0.0).astype(jnp.bfloat16)
            keys.append(jnp.concatenate([kv[unit, b, 0:tok, :], shut], axis=1))
            vt = kv[unit, b, tok : 2 * tok, :].T
            values.append(jnp.concatenate([vt, jnp.ones((16, tok), jnp.bfloat16)], axis=0))
        tiles = [(i, q) for i in range(group) for q in range(2)]

        def scores(i, q):
            right = qt[group * j + i, :, q * tok : (q + 1) * tok]
            return [jnp.dot(keys[b], right, preferred_element_type=jnp.float32) for b in range(2)]

        def summed(i, q, ps, alpha):
            pv = sum(jnp.dot(values[b], ps[b], preferred_element_type=jnp.float32) for b in range(2))
            at = slice(q * tok, (q + 1) * tok)
            acc[group * j + i, :, at] = acc[group * j + i, :, at] * alpha + pv

        AHEAD = 2
        ready = [scores(*u) for u in tiles[:AHEAD]]
        waiting = None
        for pos, (i, q) in enumerate(tiles):
            if pos + AHEAD < len(tiles):
                ready.append(scores(*tiles[pos + AHEAD]))
            ss = ready.pop(0)
            if masked is not None:
                sign, shift = masked
                diff = lax.broadcasted_iota(jnp.int32, (tok, tok), 0) - lax.broadcasted_iota(jnp.int32, (tok, tok), 1)
                ss = [jnp.where(sign * (diff + (b - q) * tok) + shift <= 0, ss[b], LOW) for b in range(2)]
            at = slice(q * tok, (q + 1) * tok)
            m_old = m_ref[group * j + i, :, at]
            m_new = m_old
            for x in ss:
                m_new = jnp.maximum(m_new, jnp.max(x, axis=0, keepdims=True))
            ps = [jnp.exp2((x - m_new) * scale).astype(jnp.bfloat16) for x in ss]
            alpha = jnp.exp2((m_old - m_new) * scale)
            m_ref[group * j + i, :, at] = m_new
            if waiting is not None:
                summed(*waiting)
            waiting = (i, q, ps, alpha)
        summed(*waiting)

    def entry(e, carry):
        op, b, mask, unit = decode(e)

        @pl.when(op == LOCAL)
        def _():
            for j in range(2):

                @pl.when(unit == here + j)
                def _(j=j):
                    for t in range(2):
                        mine[3 * j + t].wait()

        @pl.when(op == SIBLING)
        def _():
            for j in range(2):

                @pl.when(unit == here + j)
                def _(j=j):
                    for t in range(3):
                        coming(j, t).wait_recv()

        @pl.when(op == LINK)
        def _():
            link(0, unit, b).wait_recv()

        for d in range(4):

            @pl.when(lax.rem(lax.div(mask, 2**d), 2) == 1)
            def _(d=d):
                link(d, unit, b).start()

        return carry

    def step(t, carry):
        lax.fori_loop(jnp.where(t == 0, first, ends[jnp.maximum(t - 1, 0)]), ends[t], entry, 0)
        unit = pick(units, [lax.rem(lax.div(t, 2**i), 2) == 1 for i in range(steps.bit_length())])
        slab = lax.div(unit, 2)
        back, at = c - lax.div(slab, n), lax.rem(slab, n)
        rim = (at == z) & ((back == 0) | (back == 2))

        @pl.when((t < active) & rim)
        def _():
            sign = jnp.where(back == 0, 1, -1)
            body(unit, (sign, jnp.where(back == 0, 0, 1)))

        @pl.when((t < active) & jnp.logical_not(rim))
        def _():
            body(unit, None)

        return carry

    first = 4
    lax.fori_loop(0, 2, entry, 0)
    m_ref[...] = jnp.full_like(m_ref, LOW)
    acc[...] = jnp.zeros_like(acc)
    mine[6].wait()
    query_block(k)
    lax.fori_loop(2, first, entry, 0)
    for i in (6, 7):
        ref = (qraw, segs)[i - 6].at[1 - k]
        to_sib(ref, ref, i).wait_recv()
    query_block(1 - k)
    lax.fori_loop(0, steps, step, 0)
    lax.fori_loop(ends[steps - 1], ends[steps], entry, 0)

    rows = pl.ds(pl.multiple_of(k * heads, heads), heads)
    low = pl.ds(pl.multiple_of((1 - k) * heads, heads), heads)

    def strip(core, j):
        width = group * HEAD_DIM
        return pl.ds(pl.multiple_of((2 * core + j) * width, width), width)

    back, keep = [], []
    for j in range(2):
        for h in range(group * j, group * (j + 1)):
            total = acc[h, HEAD_DIM : HEAD_DIM + 1, :]
            out = acc[h, 0:HEAD_DIM, :] * (1.0 / total)
            logs = m_ref[h] * (1.0 / math.sqrt(HEAD_DIM)) + jnp.log(total)
            for b in range(2):
                at = slice(b * tok, (b + 1) * tok)
                at_h = slice((h - group * j) * HEAD_DIM, (h - group * j + 1) * HEAD_DIM)
                obuf[j, b, :, at_h] = out[:, at].astype(obuf.dtype).T
                lsbuf[b, h : h + 1, :] = logs[:, at]
        back.append(to_sib(obuf.at[j, 1 - k], o_out.at[:, strip(k, j)], (8, 10)[j]))
        keep.append(pltpu.make_async_copy(obuf.at[j, k], o_out.at[:, strip(k, j)], local.at[(8, 10)[j]]))
        back[j].start()
        keep[j].start()
    back.append(to_sib(lsbuf.at[1 - k], ls_out.at[rows, :], 9))
    keep.append(pltpu.make_async_copy(lsbuf.at[k], ls_out.at[rows, :], local.at[9]))
    back[2].start()
    keep[2].start()

    def finish(e, carry):
        w = sent[e]
        d, w = lax.rem(w, 4), lax.div(w, 4)
        ref = kv.at[lax.div(w, 2), lax.rem(lax.rem(w, 2) + k, 2)]
        pltpu.make_async_remote_copy(
            src_ref=ref, dst_ref=ref,
            send_sem=link_send.at[d, lax.div(w, 2), lax.rem(lax.rem(w, 2) + k, 2)], recv_sem=sib_recv.at[0],
            device_id=(c, sib), device_id_type=pl.DeviceIdType.MESH,
        ).wait_send()
        return carry

    lax.fori_loop(0, ends[steps + 1], finish, 0)
    for copy in theirs + back:
        copy.wait_send()
    for j in range(2):
        to_sib(obuf.at[j, k], o_out.at[:, strip(1 - k, j)], (8, 10)[j]).wait_recv()
    to_sib(lsbuf.at[k], ls_out.at[low, :], 9).wait_recv()
    for copy in keep:
        copy.wait()


def store(o_in, ls_in, o_out, ls_out, sems):
    copies = [pltpu.make_async_copy(ls_in, ls_out, sems.at[4])]
    rows = o_in.shape[0] // 4
    for i in range(4):
        at = pl.ds(i * rows, rows)
        copies.append(pltpu.make_async_copy(o_in.at[at, :], o_out.at[at, :], sems.at[i]))
    for copy in copies:
        copy.start()
    for copy in copies:
        copy.wait()


def fused(queries, key_rows, value_rows, segments):
    n = lax.axis_size("seq") // 2
    tok = queries.shape[0]
    heads = Q_HEADS // 2
    hbm = pl.BlockSpec(memory_space=pltpu.HBM)
    units = 8 * n
    moves, stops, _, _, sends = schedule(n)
    shapes = [
        jax.ShapeDtypeStruct(queries.shape, jnp.bfloat16),
        jax.ShapeDtypeStruct((Q_HEADS, tok), jnp.float32),
    ]
    held = pl.pallas_call(
        functools.partial(exchange_attend, n),
        out_shape=shapes,
        in_specs=[hbm] * 4,
        out_specs=[pl.BlockSpec(memory_space=pl.ANY)] * 2,
        scratch_shapes=[
            pltpu.SMEM((max(len(m) for m in moves),), jnp.int32),
            pltpu.SMEM((len(stops[0]) + 1,), jnp.int32),
            pltpu.SMEM((max(len(m) for m in sends),), jnp.int32),
            pltpu.VMEM((16, HEAD_DIM), jnp.bfloat16),
            pltpu.VMEM((16, tok), jnp.bfloat16),
            pltpu.VMEM((units, 2, 2 * tok + 16, HEAD_DIM), jnp.bfloat16),
            pltpu.VMEM((2, tok, heads * HEAD_DIM), jnp.bfloat16),
            pltpu.VMEM((2, 16, tok), jnp.bfloat16),
            pltpu.VMEM((heads, 2 * HEAD_DIM, 2 * tok), jnp.bfloat16),
            pltpu.VMEM((heads, 1, 2 * tok), jnp.float32),
            pltpu.VMEM((heads, HEAD_DIM + 16, 2 * tok), jnp.float32),
            pltpu.VMEM((2, 2, tok, heads // 2 * HEAD_DIM), jnp.bfloat16),
            pltpu.VMEM((2, heads, tok), jnp.float32),
            pltpu.VMEM((1, tok), jnp.int32),
            pltpu.SemaphoreType.DMA((11,)),
            pltpu.SemaphoreType.DMA((11,)),
            pltpu.SemaphoreType.DMA((11,)),
            pltpu.SemaphoreType.DMA((4, units, 2)),
            pltpu.SemaphoreType.DMA((units, 2)),
        ],
        compiler_params=pltpu.CompilerParams(
            collective_id=0, has_side_effects=True, vmem_limit_bytes=24 * 1024 * 1024
        ),
    )(*(pltpu.with_memory_space_constraint(x, pltpu.HBM) for x in (key_rows, value_rows, queries, segments[None, :])))
    anywhere = pl.BlockSpec(memory_space=pl.ANY)
    return pl.pallas_call(
        store,
        out_shape=shapes,
        in_specs=[anywhere] * 2,
        out_specs=[anywhere] * 2,
        scratch_shapes=[pltpu.SemaphoreType.DMA((5,))],
        compiler_params=pltpu.CompilerParams(vmem_limit_bytes=1024 * 1024),
    )(*held)


def on_device(queries, key_rows, value_rows, segments):
    tok = queries.shape[0]
    grp_n, seq_n = lax.axis_size("grp"), lax.axis_size("seq")
    device = lax.axis_index(AXES)
    offset = device * tok
    if grp_n == 4 and seq_n == 8 and 2 * seq_n * tok == WINDOW and tok <= 256:
        return fused(queries, key_rows, value_rows, segments)
    k_all = lax.all_gather(key_rows, AXES)
    v_all = lax.all_gather(value_rows, AXES)
    seg_all = lax.all_gather(segments, AXES)
    base = 0
    seg_all = seg_all.reshape(-1)
    key_pos = base * tok + jnp.arange(seg_all.shape[0], dtype=jnp.int32)
    begin = jnp.maximum(offset - WINDOW, 0)
    before = (key_pos >= begin) & (key_pos < offset) & (seg_all < segments[0])
    carried = begin + jnp.sum(before.astype(jnp.int32))
    inner = jnp.sum((segments[:, None] < segments[None, :]).astype(jnp.int32), axis=0)
    starts = jnp.where(segments == segments[0], carried, offset + inner)
    positions = offset + jnp.arange(tok, dtype=jnp.int32)
    lower = jnp.maximum(starts, positions - WINDOW + 1)
    first = jnp.min(lower) // tok
    clean = (jnp.max(lower) + tok - 1) // tok
    info = jnp.stack([device, first, clean, device - base]).astype(jnp.int32)
    reach = (WINDOW - 1 + tok - 1) // tok + 1
    return attention(info, lower, queries, k_all, v_all, reach)


def attention(info, lower, queries, k_all, v_all, reach):
    tok = queries.shape[0]
    width = k_all.shape[2]

    def kv_index(j, info):
        return (jnp.maximum(info[3] - j, info[3] - info[0] + info[1]), 0, 0)

    const = lambda j, info: (0, 0)
    return pl.pallas_call(
        flash,
        grid_spec=pltpu.PrefetchScalarGridSpec(
            num_scalar_prefetch=1,
            grid=(reach,),
            in_specs=[
                pl.BlockSpec((1, tok), const),
                pl.BlockSpec(queries.shape, const),
                pl.BlockSpec((None, tok, width), kv_index),
                pl.BlockSpec((None, tok, width), kv_index),
            ],
            out_specs=[
                pl.BlockSpec(queries.shape, const),
                pl.BlockSpec((Q_HEADS, tok), const),
            ],
            scratch_shapes=[
                pltpu.VMEM((Q_HEADS, HEAD_DIM, tok), jnp.bfloat16),
                pltpu.VMEM((Q_HEADS, 1, tok), jnp.float32),
                pltpu.VMEM((Q_HEADS, 1, tok), jnp.float32),
                pltpu.VMEM((Q_HEADS, HEAD_DIM, tok), jnp.float32),
                pltpu.VMEM((tok, tok), jnp.float32),
            ],
        ),
        out_shape=[
            jax.ShapeDtypeStruct(queries.shape, jnp.bfloat16),
            jax.ShapeDtypeStruct((Q_HEADS, tok), jnp.float32),
        ],
        compiler_params=pltpu.CompilerParams(dimension_semantics=("arbitrary",)),
    )(info, lower[None, :], queries, k_all, v_all)


def solution(mesh):
    in_specs = (P(AXES, None), P(AXES, None), P(AXES, None), P(AXES))
    out_specs = (P(AXES, None), P(None, AXES))
    return jax.shard_map(
        on_device, mesh=mesh, in_specs=in_specs, out_specs=out_specs, check_vma=False
    )
```

```python
import functools
import heapq
import math

import jax
import jax.numpy as jnp
from jax import lax
from jax.experimental import pallas as pl
from jax.experimental.pallas import tpu as pltpu
from jax.sharding import PartitionSpec as P

Q_HEADS = 16
KV_HEADS = 4
HEAD_DIM = 128
WINDOW = 4096
AXES = ("grp", "seq")
LOW = -1e30


def block_step(qt, k_ref, v_ref, m_ref, l_ref, acc, bias):
    c = math.log2(math.e) / math.sqrt(HEAD_DIM)
    group = Q_HEADS // KV_HEADS

    def scores(h):
        g = h // group
        return jnp.dot(
            k_ref[:, g * HEAD_DIM : (g + 1) * HEAD_DIM], qt[h], preferred_element_type=jnp.float32
        )

    def summed(h, p, alpha):
        g = h // group
        if h % group == 0:
            vts[g] = v_ref[:, g * HEAD_DIM : (g + 1) * HEAD_DIM].T
        acc[h] = acc[h] * alpha + jnp.dot(vts[g], p, preferred_element_type=jnp.float32)

    vts = {}
    AHEAD = 2
    ready = [scores(h) for h in range(AHEAD)]
    waiting = None
    for h in range(Q_HEADS):
        if h + AHEAD < Q_HEADS:
            ready.append(scores(h + AHEAD))
        s = ready.pop(0)
        if bias is not None:
            s = s + bias[...]
        m_old = m_ref[h]
        m_new = jnp.maximum(m_old, jnp.max(s, axis=0, keepdims=True))
        p = jnp.exp2((s - m_new) * c)
        alpha = jnp.exp2((m_old - m_new) * c)
        l_ref[h] = l_ref[h] * alpha + jnp.sum(p, axis=0, keepdims=True)
        m_ref[h] = m_new
        if waiting is not None:
            summed(*waiting)
        waiting = (h, p.astype(jnp.bfloat16), alpha)
    summed(*waiting)


def flash(info, lower_ref, q_ref, k_ref, v_ref, o_ref, ls_ref, qt, m_ref, l_ref, acc, bias):
    j = pl.program_id(0)
    tok = q_ref.shape[0]
    device, first, clean = info[0], info[1], info[2]

    @pl.when(j == 0)
    def _():
        for h in range(Q_HEADS):
            qt[h] = q_ref[:, h * HEAD_DIM : (h + 1) * HEAD_DIM].T
        m_ref[...] = jnp.full_like(m_ref, LOW)
        l_ref[...] = jnp.zeros_like(l_ref)
        acc[...] = jnp.zeros_like(acc)

    block = device - j
    edge = (j == 0) | (block < clean)

    @pl.when((block >= first) & edge)
    def _():
        key_pos = block * tok + lax.broadcasted_iota(jnp.int32, (tok, tok), 0)
        pos = device * tok + lax.broadcasted_iota(jnp.int32, (tok, tok), 1)
        allowed = (key_pos >= lower_ref[...]) & (key_pos <= pos)
        bias[...] = jnp.where(allowed, 0.0, LOW)
        block_step(qt, k_ref, v_ref, m_ref, l_ref, acc, bias)

    @pl.when((block >= first) & jnp.logical_not(edge))
    def _():
        block_step(qt, k_ref, v_ref, m_ref, l_ref, acc, None)

    @pl.when(j == pl.num_programs(0) - 1)
    def _():
        for h in range(Q_HEADS):
            out = acc[h] * (1.0 / l_ref[h])
            o_ref[:, h * HEAD_DIM : (h + 1) * HEAD_DIM] = out.T.astype(o_ref.dtype)
            ls_ref[h : h + 1, :] = m_ref[h] * (1.0 / math.sqrt(HEAD_DIM)) + jnp.log(l_ref[h])


ROUTES = (
    1839685, 1855310, 1758440, 1758565, 4890511576, 9650953, 8464676, 8488425, 42791646, 4929557131, 44727131,
    44816506, 122230363153, 223331905, 213541355, 213542606, 125661521875, 123237693825, 4858872225, 1099025020,
    4608094065, 18200594475, 3659955416, 125683000715, 29780628525, 29780628575, 18034925391, 24382191625,
    133541425450, 144445703125, 151057046875, 142492578125, 114378906250, 114378906250, 82642578125, 108275390625,
    83417968750, 113886718750, 100947656250, 107051171875, 111425781250, 111425781250, 99218750000, 111425781250,
    113049218750, 114269921875, 99121093750, 99121093750, 75683593750, 75683593750, 75683593750, 75683593750,
    73242187500, 73242187500, 73242187500, 73242187500, 61035156250, 61035156250, 61035156250, 61035156250, 0, 0, 0,
    0,
)
EARLY = (
    5, -3, -6.5, -2, 2.5, -5, 9.5, -2.5, -5, -7.5, 2, 9, -4, -6.5, 1, 4.5, -2, -2, 2, 1.5, -3, 0, 1, 10.5, 6, -5.5,
    -6, 0, -8, -11, -7.5, 6.5, 0.5, 1.5, -4, -10, -3, 2.5, 7.5, 4, -6.5, -5, 1.5, 1.5, -2, -5, 8, 8, -3, 11, -0.5,
    12, 6.5, -3, 8.5, 0.5, 0, -3.5, 8, -6, 4, 9.5, 3.5, -1.5,
)


def needed(c, z, g, s):
    return (g == c and s <= z) or g == c - 1 or (g == c - 2 and s >= z)


LOCAL, SIBLING, LINK, SEND, COMPUTE = range(5)


def schedule(n, chunk=2.95, flight=1.7, work=1.8, ahead=2.8, ready=5.0):
    chips = [(c, z) for c in range(4) for z in range(n)]
    near = []
    for c, z in chips:
        ways = ((c, z + 1), (c, z - 1), (c ^ 1, z), (c ^ 2, z))
        near.append([chips.index(w) if w in chips else None for w in ways])
    count = len(chips)
    home = [chip for chip in range(count) for _ in range(4)]
    kids, depth = [], []
    for code in ROUTES:
        above = []
        for chip in range(count):
            code, way = divmod(code, 5)
            above.append(near[chip][way - 1] if way else None)
        kid, deep = [[] for _ in chips], [0] * count
        for chip in range(count):
            if above[chip] is not None:
                kid[above[chip]].append(near[above[chip]].index(chip))
                far, hops = chip, 0
                while above[far] is not None:
                    far, hops = above[far], hops + 1
                    deep[far] = max(deep[far], hops)
        kids.append(kid)
        depth.append(deep)

    free = [[0.0] * 4 for _ in chips]
    pend = [[[] for _ in range(4)] for _ in chips]
    inbox = [sorted((2.0 + 1.5 * b, -j, i * 4 + j * 2 + b) for b in (0, 1) for j in (1, 0)) for i in range(count)]
    have, todo, prog = [[] for _ in chips], [[] for _ in chips], [[] for _ in chips]
    clock, order = [2.0] * count, 0

    def option(i):
        found = [(max(free[i][d] - ahead, clock[i]), 0, d) for d in range(4) if pend[i][d]]
        if inbox[i]:
            found.append((max(inbox[i][0][0], clock[i]), 1, 0))
        if todo[i]:
            found.append((max(clock[i], ready), 2, 0))
        return min(found, default=None)

    def issue(i, d, t):
        q = heapq.heappop(pend[i][d])[2]
        to = near[i][d]
        free[i][d] = max(free[i][d], t) + chunk
        heapq.heappush(inbox[to], (free[i][d] + flight, 0, q))
        choice[to] = option(to)
        return q

    choice = [option(i) for i in range(count)]
    while any(o is not None for o in choice):
        t, i = min((o[0], i) for i, o in enumerate(choice) if o is not None)
        _, kind, d = choice[i]
        if kind == 0:
            prog[i].append((SEND, issue(i, d, t), 1 << d))
            clock[i] = t + 0.07
        elif kind == 1:
            q = heapq.heappop(inbox[i])[2]
            mask = 0
            for d in kids[q][i]:
                order += 1
                heapq.heappush(pend[i][d], (-depth[q][near[i][d]] - EARLY[q], order, q))
                if free[i][d] - ahead <= t and pend[i][d][0][2] == q:
                    issue(i, d, t)
                    mask |= 1 << d
            prog[i].append((LINK if home[q] != i else (LOCAL, SIBLING)[q % 2], q, mask))
            clock[i] = t + 0.12
            have[i].append(q)
            if needed(*chips[i], *chips[home[q]]) and q ^ 1 in have[i]:
                todo[i].append(q // 2)
        else:
            todo[i].sort(key=lambda u: u // 2 != i)
            prog[i].append((COMPUTE, todo[i].pop(0) * 2, 0))
            clock[i] = t + work
        choice[i] = option(i)
    for i in range(count):
        assert len(have[i]) == len(set(have[i]))
        done = sorted(q // 2 for op, q, _ in prog[i] if op == COMPUTE)
        assert done == [u for u in range(2 * count) if needed(*chips[i], *chips[u // 2])]

    def word(op, q, mask):
        return op + 8 * (q % 2 + 2 * (mask + 16 * (q // 2)))

    moves, stops, works = [], [], []
    for entries in prog:
        stop, work = [], []
        for place, (op, q, _) in enumerate(entries):
            if op == COMPUTE:
                stop.append(place - len(work))
                work.append(q // 2)
        move = [word(*e) for e in entries if e[0] != COMPUTE]
        moves.append(move)
        stops.append(stop + [len(move)])
        works.append(work)
    steps = max(len(w) for w in works)
    counts = [len(w) for w in works]
    stops = [s[:-1] + [s[-1]] * (steps + 1 - len(s) + 1) for s in stops]
    works = [w + [w[-1]] * (steps - len(w)) for w in works]
    sends = [
        [d + 4 * (w // 8 % 2 + 2 * (w // 256)) for w in move for d in range(4) if w // 16 // 2**d % 2] for move in moves
    ]
    return moves, stops, works, counts, sends


def pick(words, bits):
    for bit in bits:
        if len(words) == 1:
            break
        pairs = [(words[i], words[min(i + 1, len(words) - 1)]) for i in range(0, len(words), 2)]
        words = [
            lo if isinstance(lo, int) and isinstance(hi, int) and lo == hi else jnp.where(bit, jnp.int32(hi), jnp.int32(lo))
            for lo, hi in pairs
        ]
    return words[0]


def exchange_attend(n, k_in, v_in, q_in, seg_in, o_out, ls_out, table, ends, sent, c_in, s_in, kv, qraw, segs, qt, m_ref, acc, obuf, lsbuf, seg_here,
                    local, sib_send, sib_recv, link_send, link_recv):
    tok = k_in.shape[0]
    heads = Q_HEADS // 2
    group = Q_HEADS // KV_HEADS
    scale = math.log2(math.e) / math.sqrt(HEAD_DIM)
    c, s = lax.axis_index("grp"), lax.axis_index("seq")
    z, k = lax.div(s, 2), lax.rem(s, 2)
    sib = s + 1 - 2 * k
    row, col = lax.div(c, 2), lax.rem(c, 2)
    peers = (
        (z + 1 < n, (c, s + 2)),
        (z > 0, (c, s - 2)),
        (c >= 0, (c + 1 - 2 * col, s)),
        (c >= 0, (c + 2 - 4 * row, s)),
        (c >= 0, (c, sib)),
    )
    here = (c * n + z) * 2

    def parts(core):
        made = []
        for j in range(2):
            cols = pl.ds(pl.multiple_of((2 * core + j) * HEAD_DIM, HEAD_DIM), HEAD_DIM)
            for t, src in enumerate((k_in.at[:, cols], v_in.at[:, cols], c_in)):
                rows = pl.ds(t * tok, src.shape[0])
                made.append((src, kv.at[here + j, k, rows, :], 3 * j + t))
        cols = pl.ds(pl.multiple_of(core * heads * HEAD_DIM, HEAD_DIM), heads * HEAD_DIM)
        made.append((q_in.at[:, cols], qraw.at[k], 6))
        made.append((s_in, segs.at[k], 7))
        return made

    def to_sib(src, dst, i):
        return pltpu.make_async_remote_copy(
            src_ref=src, dst_ref=dst, send_sem=sib_send.at[i], recv_sem=sib_recv.at[i],
            device_id=(c, sib), device_id_type=pl.DeviceIdType.MESH,
        )

    mine = {i: pltpu.make_async_copy(src, dst, local.at[i]) for src, dst, i in parts(k) if i in (0, 1, 3, 4, 6)}
    theirs = [to_sib(src, dst, i) for src, dst, i in parts(1 - k)]

    def coming(j, t):
        rows = pl.ds(t * tok, tok if t < 2 else c_in.shape[0])
        ref = kv.at[here + j, 1 - k, rows, :]
        return to_sib(ref, ref, 3 * j + t)

    fetch = pltpu.make_async_copy(seg_in, seg_here, local.at[7])
    fetch.start()
    for copy in mine.values():
        copy.start()
    barrier = pltpu.get_barrier_semaphore()
    count = 0
    for ok, to in peers:
        count = count + ok.astype(jnp.int32)

        @pl.when(ok)
        def _(to=to):
            pl.semaphore_signal(barrier, inc=1, device_id=to, device_id_type=pl.DeviceIdType.MESH)

    moves, stops, works, counts, sends = schedule(n)
    for i in range(len(moves)):

        @pl.when(c * n + z == i)
        def _(i=i):
            for e, w in enumerate(moves[i]):
                table[e] = w
            for e, w in enumerate(stops[i] + [len(sends[i])]):
                ends[e] = w
            for e, w in enumerate(sends[i]):
                sent[e] = w

    bits = [lax.rem(lax.div(c * n + z, 2**i), 2) == 1 for i in range(4)]
    steps = len(works[0])
    units = [pick([w[t] for w in works], bits) for t in range(steps)]
    active = pick(counts, bits)

    fetch.wait()
    seg = seg_here[...].astype(jnp.float32)
    docs = lax.broadcasted_iota(jnp.int32, (HEAD_DIM, tok), 0).astype(jnp.float32)
    before = jnp.where(seg < docs, 1.0, 0.0).astype(jnp.bfloat16)
    counted = lax.dot_general(
        jnp.ones((16, tok), jnp.bfloat16), before, (((1,), (1,)), ((), ())), preferred_element_type=jnp.float32
    ).astype(jnp.bfloat16)
    wide = jnp.broadcast_to(seg, (16, tok)).astype(jnp.bfloat16)
    c_in[...] = counted
    s_in[...] = wide
    segs[k] = wide
    for j in range(2):
        kv[here + j, k, 2 * tok : 2 * tok + 16, :] = counted
    pl.semaphore_wait(barrier, count)
    for copy in theirs:
        copy.start()

    def link(d, unit, b):
        return pltpu.make_async_remote_copy(
            src_ref=kv.at[unit, b], dst_ref=kv.at[unit, b],
            send_sem=link_send.at[d, unit, b], recv_sem=link_recv.at[unit, b],
            device_id=peers[d][1], device_id_type=pl.DeviceIdType.MESH,
        )

    def decode(e):
        w = table[e]
        op, w = lax.rem(w, 8), lax.div(w, 8)
        b, w = lax.rem(w, 2), lax.div(w, 2)
        mask, unit = lax.rem(w, 16), lax.div(w, 16)
        return op, lax.rem(b + k, 2), mask, unit

    def query_block(b):
        onehot = lax.broadcasted_iota(jnp.int32, (HEAD_DIM, tok), 0).astype(jnp.float32)
        onehot = (segs[b, 0:1, :].astype(jnp.float32) == onehot).astype(jnp.bfloat16)
        at = pl.ds(pl.multiple_of(b * tok, HEAD_DIM), tok)
        for h in range(heads):
            qt[h, 0:HEAD_DIM, at] = qraw[b, :, h * HEAD_DIM : (h + 1) * HEAD_DIM].T
            qt[h, HEAD_DIM:, at] = onehot

    def body(unit, masked):
        j = lax.rem(unit, 2)
        keys, values = [], []
        for b in range(2):
            counts = kv[unit, b, 2 * tok : 2 * tok + 1, :].astype(jnp.float32)
            at = lax.broadcasted_iota(jnp.int32, (tok, HEAD_DIM), 0).astype(jnp.float32)
            shut = jnp.where(at < counts, LOW, 0.0).astype(jnp.bfloat16)
            keys.append(jnp.concatenate([kv[unit, b, 0:tok, :], shut], axis=1))
            vt = kv[unit, b, tok : 2 * tok, :].T
            values.append(jnp.concatenate([vt, jnp.ones((16, tok), jnp.bfloat16)], axis=0))
        tiles = [(i, q) for q in range(2) for i in range(group)]

        def scores(i, q):
            right = qt[group * j + i, :, q * tok : (q + 1) * tok]
            return [jnp.dot(keys[b], right, preferred_element_type=jnp.float32) for b in range(2)]

        def summed(i, q, ps, alpha):
            pv = sum(jnp.dot(values[b], ps[b], preferred_element_type=jnp.float32) for b in range(2))
            at = slice(q * tok, (q + 1) * tok)
            acc[group * j + i, :, at] = acc[group * j + i, :, at] * alpha + pv

        AHEAD = 2
        ready = [scores(*u) for u in tiles[:AHEAD]]
        waiting = None
        for pos, (i, q) in enumerate(tiles):
            if pos + AHEAD < len(tiles):
                ready.append(scores(*tiles[pos + AHEAD]))
            ss = ready.pop(0)
            if masked is not None:
                sign, shift = masked
                diff = lax.broadcasted_iota(jnp.int32, (tok, tok), 0) - lax.broadcasted_iota(jnp.int32, (tok, tok), 1)
                ss = [jnp.where(sign * (diff + (b - q) * tok) + shift <= 0, ss[b], LOW) for b in range(2)]
            at = slice(q * tok, (q + 1) * tok)
            m_old = m_ref[group * j + i, :, at]
            m_new = m_old
            for x in ss:
                m_new = jnp.maximum(m_new, jnp.max(x, axis=0, keepdims=True))
            ps = [jnp.exp2((x - m_new) * scale).astype(jnp.bfloat16) for x in ss]
            alpha = jnp.exp2((m_old - m_new) * scale)
            m_ref[group * j + i, :, at] = m_new
            if waiting is not None:
                summed(*waiting)
            waiting = (i, q, ps, alpha)
        summed(*waiting)

    def entry(e, carry):
        op, b, mask, unit = decode(e)

        @pl.when(op == LOCAL)
        def _():
            for j in range(2):

                @pl.when(unit == here + j)
                def _(j=j):
                    for t in range(2):
                        mine[3 * j + t].wait()

        @pl.when(op == SIBLING)
        def _():
            for j in range(2):

                @pl.when(unit == here + j)
                def _(j=j):
                    for t in range(3):
                        coming(j, t).wait_recv()

        @pl.when(op == LINK)
        def _():
            link(0, unit, b).wait_recv()

        for d in range(4):

            @pl.when(lax.rem(lax.div(mask, 2**d), 2) == 1)
            def _(d=d):
                link(d, unit, b).start()

        return carry

    def step(t, carry):
        lax.fori_loop(jnp.where(t == 0, first, ends[jnp.maximum(t - 1, 0)]), ends[t], entry, 0)
        unit = pick(units, [lax.rem(lax.div(t, 2**i), 2) == 1 for i in range(steps.bit_length())])
        slab = lax.div(unit, 2)
        back, at = c - lax.div(slab, n), lax.rem(slab, n)
        rim = (at == z) & ((back == 0) | (back == 2))

        @pl.when((t < active) & rim)
        def _():
            sign = jnp.where(back == 0, 1, -1)
            body(unit, (sign, jnp.where(back == 0, 0, 1)))

        @pl.when((t < active) & jnp.logical_not(rim))
        def _():
            body(unit, None)

        return carry

    first = 4
    lax.fori_loop(0, 2, entry, 0)
    m_ref[...] = jnp.full_like(m_ref, LOW)
    acc[...] = jnp.zeros_like(acc)
    mine[6].wait()
    query_block(k)
    lax.fori_loop(2, first, entry, 0)
    for i in (6, 7):
        ref = (qraw, segs)[i - 6].at[1 - k]
        to_sib(ref, ref, i).wait_recv()
    query_block(1 - k)
    lax.fori_loop(0, steps, step, 0)
    lax.fori_loop(ends[steps - 1], ends[steps], entry, 0)

    rows = pl.ds(pl.multiple_of(k * heads, heads), heads)
    low = pl.ds(pl.multiple_of((1 - k) * heads, heads), heads)

    def strip(core, j):
        width = group * HEAD_DIM
        return pl.ds(pl.multiple_of((2 * core + j) * width, width), width)

    back, keep = [], []
    for j in range(2):
        for h in range(group * j, group * (j + 1)):
            total = acc[h, HEAD_DIM : HEAD_DIM + 1, :]
            out = acc[h, 0:HEAD_DIM, :] * (1.0 / total)
            logs = m_ref[h] * (1.0 / math.sqrt(HEAD_DIM)) + jnp.log(total)
            for b in range(2):
                at = slice(b * tok, (b + 1) * tok)
                at_h = slice((h - group * j) * HEAD_DIM, (h - group * j + 1) * HEAD_DIM)
                obuf[j, b, :, at_h] = out[:, at].astype(obuf.dtype).T
                lsbuf[b, h : h + 1, :] = logs[:, at]
        back.append(to_sib(obuf.at[j, 1 - k], o_out.at[:, strip(k, j)], (8, 10)[j]))
        keep.append(pltpu.make_async_copy(obuf.at[j, k], o_out.at[:, strip(k, j)], local.at[(8, 10)[j]]))
        back[j].start()
        keep[j].start()
    back.append(to_sib(lsbuf.at[1 - k], ls_out.at[rows, :], 9))
    keep.append(pltpu.make_async_copy(lsbuf.at[k], ls_out.at[rows, :], local.at[9]))
    back[2].start()
    keep[2].start()

    def finish(e, carry):
        w = sent[e]
        d, w = lax.rem(w, 4), lax.div(w, 4)
        ref = kv.at[lax.div(w, 2), lax.rem(lax.rem(w, 2) + k, 2)]
        pltpu.make_async_remote_copy(
            src_ref=ref, dst_ref=ref,
            send_sem=link_send.at[d, lax.div(w, 2), lax.rem(lax.rem(w, 2) + k, 2)], recv_sem=sib_recv.at[0],
            device_id=(c, sib), device_id_type=pl.DeviceIdType.MESH,
        ).wait_send()
        return carry

    lax.fori_loop(0, ends[steps + 1], finish, 0)
    for copy in theirs + back:
        copy.wait_send()
    for j in range(2):
        to_sib(obuf.at[j, k], o_out.at[:, strip(1 - k, j)], (8, 10)[j]).wait_recv()
    to_sib(lsbuf.at[k], ls_out.at[low, :], 9).wait_recv()
    for copy in keep:
        copy.wait()


def store(o_in, ls_in, o_out, ls_out, sems):
    copies = [pltpu.make_async_copy(ls_in, ls_out, sems.at[4])]
    rows = o_in.shape[0] // 4
    for i in range(4):
        at = pl.ds(i * rows, rows)
        copies.append(pltpu.make_async_copy(o_in.at[at, :], o_out.at[at, :], sems.at[i]))
    for copy in copies:
        copy.start()
    for copy in copies:
        copy.wait()


def fused(queries, key_rows, value_rows, segments):
    n = lax.axis_size("seq") // 2
    tok = queries.shape[0]
    heads = Q_HEADS // 2
    hbm = pl.BlockSpec(memory_space=pltpu.HBM)
    units = 8 * n
    moves, stops, _, _, sends = schedule(n)
    shapes = [
        jax.ShapeDtypeStruct(queries.shape, jnp.bfloat16),
        jax.ShapeDtypeStruct((Q_HEADS, tok), jnp.float32),
    ]
    held = pl.pallas_call(
        functools.partial(exchange_attend, n),
        out_shape=shapes,
        in_specs=[hbm] * 4,
        out_specs=[pl.BlockSpec(memory_space=pl.ANY)] * 2,
        scratch_shapes=[
            pltpu.SMEM((max(len(m) for m in moves),), jnp.int32),
            pltpu.SMEM((len(stops[0]) + 1,), jnp.int32),
            pltpu.SMEM((max(len(m) for m in sends),), jnp.int32),
            pltpu.VMEM((16, HEAD_DIM), jnp.bfloat16),
            pltpu.VMEM((16, tok), jnp.bfloat16),
            pltpu.VMEM((units, 2, 2 * tok + 16, HEAD_DIM), jnp.bfloat16),
            pltpu.VMEM((2, tok, heads * HEAD_DIM), jnp.bfloat16),
            pltpu.VMEM((2, 16, tok), jnp.bfloat16),
            pltpu.VMEM((heads, 2 * HEAD_DIM, 2 * tok), jnp.bfloat16),
            pltpu.VMEM((heads, 1, 2 * tok), jnp.float32),
            pltpu.VMEM((heads, HEAD_DIM + 16, 2 * tok), jnp.float32),
            pltpu.VMEM((2, 2, tok, heads // 2 * HEAD_DIM), jnp.bfloat16),
            pltpu.VMEM((2, heads, tok), jnp.float32),
            pltpu.VMEM((1, tok), jnp.int32),
            pltpu.SemaphoreType.DMA((11,)),
            pltpu.SemaphoreType.DMA((11,)),
            pltpu.SemaphoreType.DMA((11,)),
            pltpu.SemaphoreType.DMA((4, units, 2)),
            pltpu.SemaphoreType.DMA((units, 2)),
        ],
        compiler_params=pltpu.CompilerParams(
            collective_id=0, has_side_effects=True, vmem_limit_bytes=24 * 1024 * 1024
        ),
    )(*(pltpu.with_memory_space_constraint(x, pltpu.HBM) for x in (key_rows, value_rows, queries, segments[None, :])))
    anywhere = pl.BlockSpec(memory_space=pl.ANY)
    return pl.pallas_call(
        store,
        out_shape=shapes,
        in_specs=[anywhere] * 2,
        out_specs=[anywhere] * 2,
        scratch_shapes=[pltpu.SemaphoreType.DMA((5,))],
        compiler_params=pltpu.CompilerParams(vmem_limit_bytes=1024 * 1024),
    )(*held)


def on_device(queries, key_rows, value_rows, segments):
    tok = queries.shape[0]
    grp_n, seq_n = lax.axis_size("grp"), lax.axis_size("seq")
    device = lax.axis_index(AXES)
    offset = device * tok
    if grp_n == 4 and seq_n == 8 and 2 * seq_n * tok == WINDOW and tok <= 256:
        return fused(queries, key_rows, value_rows, segments)
    k_all = lax.all_gather(key_rows, AXES)
    v_all = lax.all_gather(value_rows, AXES)
    seg_all = lax.all_gather(segments, AXES)
    base = 0
    seg_all = seg_all.reshape(-1)
    key_pos = base * tok + jnp.arange(seg_all.shape[0], dtype=jnp.int32)
    begin = jnp.maximum(offset - WINDOW, 0)
    before = (key_pos >= begin) & (key_pos < offset) & (seg_all < segments[0])
    carried = begin + jnp.sum(before.astype(jnp.int32))
    inner = jnp.sum((segments[:, None] < segments[None, :]).astype(jnp.int32), axis=0)
    starts = jnp.where(segments == segments[0], carried, offset + inner)
    positions = offset + jnp.arange(tok, dtype=jnp.int32)
    lower = jnp.maximum(starts, positions - WINDOW + 1)
    first = jnp.min(lower) // tok
    clean = (jnp.max(lower) + tok - 1) // tok
    info = jnp.stack([device, first, clean, device - base]).astype(jnp.int32)
    reach = (WINDOW - 1 + tok - 1) // tok + 1
    return attention(info, lower, queries, k_all, v_all, reach)


def attention(info, lower, queries, k_all, v_all, reach):
    tok = queries.shape[0]
    width = k_all.shape[2]

    def kv_index(j, info):
        return (jnp.maximum(info[3] - j, info[3] - info[0] + info[1]), 0, 0)

    const = lambda j, info: (0, 0)
    return pl.pallas_call(
        flash,
        grid_spec=pltpu.PrefetchScalarGridSpec(
            num_scalar_prefetch=1,
            grid=(reach,),
            in_specs=[
                pl.BlockSpec((1, tok), const),
                pl.BlockSpec(queries.shape, const),
                pl.BlockSpec((None, tok, width), kv_index),
                pl.BlockSpec((None, tok, width), kv_index),
            ],
            out_specs=[
                pl.BlockSpec(queries.shape, const),
                pl.BlockSpec((Q_HEADS, tok), const),
            ],
            scratch_shapes=[
                pltpu.VMEM((Q_HEADS, HEAD_DIM, tok), jnp.bfloat16),
                pltpu.VMEM((Q_HEADS, 1, tok), jnp.float32),
                pltpu.VMEM((Q_HEADS, 1, tok), jnp.float32),
                pltpu.VMEM((Q_HEADS, HEAD_DIM, tok), jnp.float32),
                pltpu.VMEM((tok, tok), jnp.float32),
            ],
        ),
        out_shape=[
            jax.ShapeDtypeStruct(queries.shape, jnp.bfloat16),
            jax.ShapeDtypeStruct((Q_HEADS, tok), jnp.float32),
        ],
        compiler_params=pltpu.CompilerParams(dimension_semantics=("arbitrary",)),
    )(info, lower[None, :], queries, k_all, v_all)


def solution(mesh):
    in_specs = (P(AXES, None), P(AXES, None), P(AXES, None), P(AXES))
    out_specs = (P(AXES, None), P(None, AXES))
    return jax.shard_map(
        on_device, mesh=mesh, in_specs=in_specs, out_specs=out_specs, check_vma=False
    )
```
